32 devices in a mesh: rows: 8 (over z, y), vecs: 4 (over x, core).
Axes of the slice: x: 2, y: 2, z: 4, core: 2. Of those that a mesh axis runs over, the one named last changes fastest.
Arguments:
- basis: bfloat16 [100, 524288], P('vecs', 'rows'), may hold values from -6 to 6
- coefficients: bfloat16 [100, 40], replicated, may hold values from -0.625 to 0.625
- eigen_values: float32 [40], P('vecs'), may hold values from -3 to 1
- stiffness: float32 [524288], P('rows'), may hold values from 6.5 to 10
- damping: float32 [524288], P('rows'), may hold values from 0.2 to 2
- mass: float32 [524288], P('rows'), may hold values from 0.5 to 2
- link_count: int32 [8], P('rows'), may hold values from 1024 to 4096, as said below
- lower_cells: int32 [8, 4096], P('rows'), may hold values from 0 to 4095
- upper_cells: int32 [8, 4096], P('rows'), may hold values from 0 to 4095
Outputs:
- eigvecs: bfloat16 [40, 524288], P('vecs', 'rows')
- residuals: bfloat16 [40, 524288], P('vecs', 'rows')
- relative_norms: float32 [40], P('vecs')
The draws below stay inside these ranges and needn't reach their ends.
Inputs may be any that keep to these rules, and one draw needn't show every extreme that they name: Interface s joins subdomain s to subdomain (s + 1) mod 8; only its first link_count[s] slots are used, the others are to be ignored. Some interface uses all 4096 slots in every draw. `lower_cells`: slots beyond link_count[s] hold values that are not used. `upper_cells`: slots beyond link_count[s] hold values that are not used.
All inputs are finite; a program needn't handle non-finite values.
Results may differ from the reference program's by a relative error of at most 0.0037.
The reference program's roundings to bfloat16 on the way count: a program that leaves them out, or rounds other values in their place, can miss the bound.
Values may be sent and summed in bfloat16 or wider, within the bound.
A program may use at most 320 MiB of HBM per device.

```python
import math
import jax
import jax.numpy as jnp
from jax import lax

RANK = 100
NV = 40
WID = 64
ZD = 16
HMAX = 4096
NSUB = 8
NROWS = 524288
N_ROWS = 8


def draw_link_count(key, part):
    first_key, second_key = jax.random.split(jax.random.fold_in(key, 17))
    counts = jax.random.randint(first_key, (NSUB,), HMAX // 4, HMAX + 1)
    chosen = jax.random.randint(second_key, (), 0, NSUB)
    return jnp.where(jnp.arange(NSUB) == chosen, HMAX, counts).astype(jnp.int32)


def place_ends(array, key, least, largest):
    shape = array.shape
    place = [jax.random.randint(jax.random.fold_in(key, axis), (), 0, shape[axis]) for axis in range(len(shape))]
    array = array.at[tuple(place)].set(least)
    longest = shape.index(max(shape))
    place[longest] = (place[longest] + 1) % shape[longest]
    return array.at[tuple(place)].set(largest)


def block_levels(rng, dims, cuts, smallest, top_value):
    gain, own = 1.0, jax.random.fold_in(rng, 6)
    for dim, blocks in cuts:
        steps = jnp.exp(jax.random.uniform(jax.random.fold_in(own, dim), (blocks,), jnp.float32, smallest / len(cuts), top_value / len(cuts)))
        gain = gain * jnp.repeat(steps, dims[dim] // blocks).reshape([-1 if axis == dim else 1 for axis in range(len(dims))])
    return gain


def scatter_about(stream_key, dims, deviation, reach, cuts=(), held_as=jnp.bfloat16):
    result = deviation * jax.random.normal(stream_key, dims, jnp.float32)
    if cuts:
        result = result * block_levels(stream_key, dims, cuts, -0.22, 0.18)
    return jnp.clip(result, -reach, reach).astype(held_as)


def setup_inputs(seed: int = 0) -> dict:
    keys = jax.random.split(jax.random.key(seed), 10)
    basis = scatter_about(keys[0], (RANK, NROWS), 1.0, 6.0, ((0, 4), (1, 8)))
    coefficients = scatter_about(keys[1], (RANK, NV), RANK ** -0.5, 0.625)
    eigen_values = jnp.clip(-3.0 + 4.0 * jax.random.uniform(keys[2], (NV,), jnp.float32) ** block_levels(keys[2], (NV,), ((0, 4),), -0.2, 0.2), -3.0, 1.0)
    stiffness = jnp.clip(6.5 + 3.5 * jax.random.uniform(keys[3], (NROWS,), jnp.float32) ** block_levels(keys[3], (NROWS,), ((0, 8),), -0.2, 0.2), 6.5, 10.0)
    damping = jnp.clip(0.2 + 1.8 * jax.random.uniform(keys[4], (NROWS,), jnp.float32) ** block_levels(keys[4], (NROWS,), ((0, 8),), -0.2, 0.2), 0.2, 2.0)
    mass = jnp.clip(jnp.exp(math.log(2.0) - 1.3862944 * jax.random.uniform(keys[5], (NROWS,), jnp.float32) ** block_levels(keys[5], (NROWS,), ((0, 8),), -0.2, 0.2)), 0.5, 2.0)
    link_count = draw_link_count(jax.random.fold_in(keys[9], 71), 0)
    lower_cells = place_ends(jax.random.randint(keys[7], (NSUB, HMAX), 0, WID * WID), jax.random.fold_in(keys[7], 1), 0, (WID * WID) - 1).astype(jnp.int32)
    upper_cells = place_ends(jax.random.randint(keys[8], (NSUB, HMAX), 0, WID * WID), jax.random.fold_in(keys[8], 1), 0, (WID * WID) - 1).astype(jnp.int32)
    return {"basis": basis, "coefficients": coefficients, "eigen_values": eigen_values, "stiffness": stiffness, "damping": damping, "mass": mass, "link_count": link_count, "lower_cells": lower_cells, "upper_cells": upper_cells}


def neighbours(values, width_cells):
    depth_pad = jnp.pad(values, ((0, 0), (1, 1), (0, 0)))
    total = depth_pad[:, 2:] + depth_pad[:, :-2]
    across = jnp.pad(values, ((0, 0), (0, 0), (width_cells, width_cells)))
    total = total + across[:, :, 2 * width_cells:] + across[:, :, :-2 * width_cells]
    column = jnp.arange(values.shape[2]) % width_cells
    shifted = jnp.pad(values, ((0, 0), (0, 0), (1, 1)))
    total = total + jnp.where(column < width_cells - 1, shifted[:, :, 2:], 0.0)
    total = total + jnp.where(column > 0, shifted[:, :, :-2], 0.0)
    return total

def reference(basis, coefficients, eigen_values, stiffness, damping, mass, link_count, lower_cells, upper_cells):
    eigvecs = jnp.dot(coefficients.T, basis, preferred_element_type=jnp.float32).astype(jnp.bfloat16)
    vectors = eigvecs.astype(jnp.float32)
    plane_cells = WID * WID
    rows_local = ZD * plane_cells
    subdomains = N_ROWS
    neighbour_sum = neighbours(vectors.reshape(NV * subdomains, ZD, plane_cells), WID).reshape(NV, subdomains * rows_local)
    index_sub = jnp.arange(subdomains, dtype=jnp.int32)[:, None]
    lower_rows = (index_sub * rows_local + (ZD - 1) * plane_cells + lower_cells).reshape(-1).astype(jnp.int32)
    upper_rows = ((index_sub + 1) % subdomains * rows_local + upper_cells).reshape(-1).astype(jnp.int32)
    slot_used = (jnp.arange(HMAX, dtype=jnp.int32)[None, :] < link_count[:, None]).astype(jnp.float32).reshape(-1)
    link_sum = jnp.zeros_like(vectors)
    link_sum = link_sum.at[:, lower_rows].add(vectors[:, upper_rows] * slot_used)
    link_sum = link_sum.at[:, upper_rows].add(vectors[:, lower_rows] * slot_used)
    eigen_col = eigen_values[:, None]
    diagonal = eigen_col * eigen_col * mass[None, :] + eigen_col * damping[None, :] + stiffness[None, :]
    coupling = eigen_col * eigen_col * 0.1 + eigen_col * 0.3 + 1.0
    residual_full = diagonal * vectors - coupling * (neighbour_sum + link_sum)
    vector_sq = lax.optimization_barrier(jnp.sum(vectors * vectors, axis=1))
    residual_sq = lax.optimization_barrier(jnp.sum(residual_full * residual_full, axis=1))
    relative_norms = jnp.sqrt(residual_sq) / jnp.sqrt(vector_sq + 1.0)
    return (eigvecs, residual_full.astype(jnp.bfloat16), relative_norms)
```

```python
import functools

import jax
import jax.numpy as jnp
from jax import lax
from jax.experimental import pallas as pl
from jax.experimental.pallas import tpu as pltpu
from jax.sharding import PartitionSpec as P

WID = 64
LANES = 128
PAD = 16
BLOCK = 512
FULL = 8


def remote(src, dst, send_sem, recv_sem, where):
    return pltpu.make_async_remote_copy(
        src_ref=src,
        dst_ref=dst,
        send_sem=send_sem,
        recv_sem=recv_sem,
        device_id=where,
        device_id_type=pl.DeviceIdType.MESH,
    )


def kernel(
    count,
    planes,
    cells,
    vector_part,
    basis,
    factors,
    eigen,
    stiffness,
    damping,
    mass,
    links,
    eig_out,
    res_out,
    norm_out,
    own_basis,
    mate_basis,
    wire_out,
    wire_in,
    values,
    face_out,
    face_in,
    links_in,
    link_sums,
    link_part,
    stat_out,
    stat_in,
    local_sem,
    mate_send,
    mate_recv,
    wire_send,
    wire_recv,
    face_send,
    face_recv,
    stat_send,
    stat_recv,
):
    row = lax.axis_index("rows")
    vec = lax.axis_index("vecs")
    mate = {"vecs": vec + 1 - 2 * (vec % 2)}
    across = {"vecs": (vec + 2) % 4}
    above = {"rows": (row + 1) % count}
    below = {"rows": (row + count - 1) % count}
    half = cells // 2
    eighth = cells // 8
    slots = links.shape[1]

    def plane_at(step):
        return (step + planes - 1) % planes

    def lanes_of(plane):
        return pl.ds(pl.multiple_of(plane * cells, cells), cells)

    def local_copy(plane):
        return pltpu.make_async_copy(
            basis.at[:, lanes_of(plane)], own_basis.at[:, lanes_of(plane)], local_sem.at[plane]
        )

    def mate_copy(plane):
        return remote(
            basis.at[:, lanes_of(plane)],
            mate_basis.at[:, lanes_of(plane)],
            mate_send.at[plane],
            mate_recv.at[plane],
            mate,
        )

    def wire_copy(plane):
        return remote(
            wire_out.at[plane], wire_in.at[plane], wire_send.at[plane], wire_recv.at[plane], across
        )

    def face_copy(which):
        return remote(
            face_out.at[which],
            face_in.at[which],
            face_send.at[which],
            face_recv.at[which],
            above if which == 0 else below,
        )

    def links_copy():
        return remote(links, links_in, face_send.at[2], face_recv.at[2], above)

    def stat_copy(step):
        return remote(
            stat_out,
            stat_in.at[step],
            stat_send.at[step],
            stat_recv.at[step],
            {"rows": (row + step) % count},
        )

    def each(first, last, body):
        def run(step, carry):
            body(step)
            return carry

        lax.fori_loop(first, last, run, 0)

    each(0, planes, lambda step: local_copy(plane_at(step)).start())

    barrier = pltpu.get_barrier_semaphore()

    def greet(where):
        pl.semaphore_signal(barrier, inc=1, device_id=where, device_id_type=pl.DeviceIdType.MESH)

    greet(mate)
    greet(across)
    each(1, count, lambda step: greet({"rows": (row + step) % count}))
    pl.semaphore_wait(barrier, count + 1)

    each(0, planes, lambda step: mate_copy(plane_at(step)).start())
    links_copy().start()

    values[...] = jnp.zeros_like(values)
    row_iota = lax.broadcasted_iota(jnp.int32, (FULL, eighth), 0)
    rest = row_iota < vector_part - FULL

    def produce(step):
        plane = plane_at(step)
        local_copy(plane).wait()
        mate_copy(plane).wait_recv()
        both = jnp.dot(
            factors[0], own_basis[:, lanes_of(plane)], preferred_element_type=jnp.float32
        ) + jnp.dot(factors[1], mate_basis[:, lanes_of(plane)], preferred_element_type=jnp.float32)
        values[plane + 1, :, LANES : LANES + cells] = both[:PAD]
        top = both[PAD : PAD + FULL]
        tail = both[PAD + FULL :]
        wire_out[plane, :, :half] = jnp.concatenate([top[:, :half], top[:, half:]], axis=0).astype(
            jnp.bfloat16
        )
        packed = []
        for side in range(2):
            total = None
            for part in range(4):
                start = (4 * side + part) * eighth
                piece = tail[:, start : start + eighth]
                if part:
                    piece = pltpu.roll(piece, 2 * part, 0)
                total = piece if total is None else total + piece
            packed.append(total)
        wire_out[plane, :, half:] = jnp.concatenate(packed, axis=0).astype(jnp.bfloat16)
        wire_copy(plane).start()

    each(0, planes, produce)

    stat_out[...] = jnp.zeros_like(stat_out)

    def fold(block):
        total = block[:, :LANES]
        for start in range(LANES, block.shape[1], LANES):
            total = total + block[:, start : start + LANES]
        return total

    def finish(plane):
        wire_copy(plane).wait_recv()
        squares = jnp.zeros((PAD, LANES), jnp.float32)
        for part in range(8):
            side = part // 4
            lanes = slice(LANES + part * eighth, LANES + (part + 1) * eighth)
            inner = (part % 4) * eighth
            top = wire_in[plane, :, inner : inner + eighth].astype(jnp.float32)
            top = top[side * FULL : (side + 1) * FULL]
            tail = wire_in[plane, :, half:].astype(jnp.float32)
            tail = tail[side * FULL : (side + 1) * FULL]
            if part % 4:
                tail = pltpu.roll(tail, FULL - 2 * (part % 4), 0)
            tail = jnp.where(rest, tail, 0.0)
            held = values[plane + 1, :, lanes] + jnp.concatenate([top, tail], axis=0)
            rounded = held.astype(jnp.bfloat16)
            exact = rounded.astype(jnp.float32)
            values[plane + 1, :, lanes] = exact
            start = pl.multiple_of(plane * cells + part * eighth, eighth)
            eig_out[:, pl.ds(start, eighth)] = rounded[:vector_part]
            squares = squares + fold(exact * exact)
        stat_out[:PAD] += squares

    lam = eigen[...]
    lam_b = jnp.broadcast_to(lam, (PAD, LANES))
    lam_sq = jnp.tile(lam_b * lam_b, (1, BLOCK // LANES))
    lam_b = jnp.tile(lam_b, (1, BLOCK // LANES))
    coupling = lam_sq * 0.1 + lam_b * 0.3 + 1.0
    column = lax.broadcasted_iota(jnp.int32, (PAD, BLOCK), 1) % WID
    wide = BLOCK + 2 * LANES

    def stencil(plane, link):
        squares = jnp.zeros((PAD, LANES), jnp.float32)
        for start in range(0, cells, BLOCK):
            inner = slice(LANES + start, LANES + start + BLOCK)
            around = values[plane + 1, :, start : start + wide]
            mid = around[:, LANES : LANES + BLOCK]

            def moved(amount):
                return pltpu.roll(around, amount % wide, 1)[:, LANES : LANES + BLOCK]

            total = values[plane, :, inner] + values[plane + 2, :, inner]
            total = total + (moved(WID) + moved(-WID))
            total = total + jnp.where(column < WID - 1, moved(-1), 0.0)
            total = total + jnp.where(column > 0, moved(1), 0.0)
            if link is not None:
                total = total + link_sums[link, :, start : start + BLOCK]
            at = pl.ds(pl.multiple_of(plane * cells + start, BLOCK), BLOCK)
            diagonal = lam_sq * mass[:, at] + lam_b * damping[:, at] + stiffness[:, at]
            full = diagonal * mid - coupling * total
            res_out[:, at] = full.astype(jnp.bfloat16)[:vector_part]
            squares = squares + fold(full * full)
        stat_out[PAD:] += squares

    tiles = cells // LANES

    def link_side(which, lists, source_row, target_row):
        stacked = jnp.concatenate(
            [face_in[which, :, t * LANES : (t + 1) * LANES] for t in range(tiles)], axis=0
        )
        link_part[...] = jnp.zeros_like(link_part)
        low_iota = lax.broadcasted_iota(jnp.int32, (LANES, BLOCK), 0)

        def some(step):
            at = pl.ds(pl.multiple_of(step * BLOCK, BLOCK), BLOCK)
            source = lists[source_row : source_row + 1, at]
            target = lists[target_row : target_row + 1, at]
            low = jnp.where(low_iota == source % LANES, 1.0, 0.0).astype(jnp.bfloat16)
            picked = jnp.dot(stacked, low, preferred_element_type=jnp.float32)
            high = jnp.broadcast_to(source // LANES, (PAD, BLOCK))
            got = jnp.zeros((PAD, BLOCK), jnp.float32)
            for t in range(tiles):
                got = got + jnp.where(high == t, picked[t * PAD : (t + 1) * PAD], 0.0)
            high = jnp.broadcast_to(target // LANES, (PAD, BLOCK))
            spread = jnp.concatenate(
                [jnp.where(high == t, got, 0.0).astype(jnp.bfloat16) for t in range(tiles)], axis=0
            )
            low = jnp.where(low_iota == target % LANES, 1.0, 0.0).astype(jnp.bfloat16)
            link_part[...] += lax.dot_general(
                spread, low, (((1,), (1,)), ((), ())), preferred_element_type=jnp.float32
            )

        each(0, slots // BLOCK, some)
        for t in range(tiles):
            link_sums[which, :, t * LANES : (t + 1) * LANES] = link_part[t * PAD : (t + 1) * PAD]

    def send_face(which, plane):
        face_out[which] = values[plane + 1, :, LANES : LANES + cells].astype(jnp.bfloat16)
        face_copy(which).start()

    finish(planes - 1)
    send_face(0, planes - 1)
    finish(0)
    send_face(1, 0)
    finish(1)

    def advance(plane):
        finish(plane)
        stencil(plane - 1, None)

    middle = max(2, planes // 2 - 1)
    each(2, middle, advance)
    face_copy(0).wait_recv()
    links_copy().wait_recv()
    link_side(0, links_in, 0, 1)
    face_copy(1).wait_recv()
    link_side(1, links, 1, 0)
    stencil(0, 0)
    each(middle, planes - 1, advance)
    stencil(planes - 2, None)
    stencil(planes - 1, 1)

    each(1, count, lambda step: stat_copy(step).start())
    stat_in[0] = stat_out[...]
    each(1, count, lambda step: stat_copy(step).wait_recv())
    total = stat_in[0]
    for step in range(1, count):
        total = total + stat_in[step]
    sums = jnp.sum(total, axis=1, keepdims=True)
    norms = jnp.sqrt(sums[PAD:]) / jnp.sqrt(sums[:PAD] + 1.0)
    norm_out[...] = jnp.broadcast_to(norms, norm_out.shape)

    each(0, planes, lambda plane: mate_copy(plane).wait_send())
    each(0, planes, lambda plane: wire_copy(plane).wait_send())
    links_copy().wait_send()
    face_copy(0).wait_send()
    face_copy(1).wait_send()
    each(1, count, lambda step: stat_copy(step).wait_send())


def on_device(
    basis,
    coefficients,
    eigen_values,
    stiffness,
    damping,
    mass,
    link_count,
    lower_cells,
    upper_cells,
):
    count = lax.axis_size("rows")
    vec = lax.axis_index("vecs")
    vector_part = eigen_values.shape[0]
    rank_part, rows_local = basis.shape
    cells = WID * WID
    planes = rows_local // cells
    slots = lower_cells.shape[1]
    mate = vec + 1 - 2 * (vec % 2)
    across = (vec + 2) % 4

    def factor(rank_owner, vector_owner):
        piece = lax.dynamic_slice(
            coefficients,
            (rank_owner * rank_part, vector_owner * vector_part),
            (rank_part, vector_part),
        )
        return jnp.pad(piece.T, ((0, PAD - vector_part), (0, 0)))

    factors = jnp.stack(
        [
            jnp.concatenate([factor(owner, vec), factor(owner, across)], axis=0)
            for owner in (vec, mate)
        ]
    )
    eigen = jnp.pad(eigen_values, (0, PAD - vector_part))[:, None]
    used = jnp.arange(slots, dtype=jnp.int32) < link_count[0]
    links = jnp.where(used[None, :], jnp.concatenate([lower_cells, upper_cells]), -1)
    links = jnp.pad(links, ((0, 6), (0, 0)), constant_values=-1)
    vmem = pl.BlockSpec(memory_space=pltpu.VMEM)
    wire = cells // 2 + cells // 8
    dma = pltpu.SemaphoreType.DMA
    eigvecs, residuals, norms = pl.pallas_call(
        functools.partial(kernel, count, planes, cells, vector_part),
        out_shape=(
            jax.ShapeDtypeStruct((vector_part, rows_local), jnp.bfloat16),
            jax.ShapeDtypeStruct((vector_part, rows_local), jnp.bfloat16),
            jax.ShapeDtypeStruct((PAD, LANES), jnp.float32),
        ),
        in_specs=[pl.BlockSpec(memory_space=pl.ANY)] + [vmem] * 6,
        out_specs=(vmem, vmem, vmem),
        scratch_shapes=[
            pltpu.VMEM((rank_part, rows_local), jnp.bfloat16),
            pltpu.VMEM((rank_part, rows_local), jnp.bfloat16),
            pltpu.VMEM((planes, PAD, wire), jnp.bfloat16),
            pltpu.VMEM((planes, PAD, wire), jnp.bfloat16),
            pltpu.VMEM((planes + 2, PAD, cells + 2 * LANES), jnp.float32),
            pltpu.VMEM((2, PAD, cells), jnp.bfloat16),
            pltpu.VMEM((2, PAD, cells), jnp.bfloat16),
            pltpu.VMEM((8, slots), jnp.int32),
            pltpu.VMEM((2, PAD, cells), jnp.float32),
            pltpu.VMEM((cells // LANES * PAD, LANES), jnp.float32),
            pltpu.VMEM((2 * PAD, LANES), jnp.float32),
            pltpu.VMEM((count, 2 * PAD, LANES), jnp.float32),
            dma((planes,)),
            dma((planes,)),
            dma((planes,)),
            dma((planes,)),
            dma((planes,)),
            dma((3,)),
            dma((3,)),
            dma((count,)),
            dma((count,)),
        ],
        compiler_params=pltpu.CompilerParams(
            collective_id=0, has_side_effects=True, vmem_limit_bytes=56 * 1024 * 1024
        ),
    )(
        basis,
        factors,
        eigen,
        stiffness[None, :],
        damping[None, :],
        mass[None, :],
        links,
    )
    return eigvecs, residuals, norms[:vector_part, 0]


def solution(mesh):
    placed = (
        P("vecs", "rows"),
        P(),
        P("vecs"),
        P("rows"),
        P("rows"),
        P("rows"),
        P("rows"),
        P("rows", None),
        P("rows", None),
    )
    return jax.shard_map(
        on_device,
        mesh=mesh,
        in_specs=placed,
        out_specs=(P("vecs", "rows"), P("vecs", "rows"), P("vecs")),
        check_vma=False,
    )
```

```python
import functools

import jax
import jax.numpy as jnp
from jax import lax
from jax.experimental import pallas as pl
from jax.experimental.pallas import tpu as pltpu
from jax.sharding import PartitionSpec as P

WID = 64
LANES = 128
PAD = 16
BLOCK = 512
FULL = 8


def remote(src, dst, send_sem, recv_sem, where):
    return pltpu.make_async_remote_copy(
        src_ref=src,
        dst_ref=dst,
        send_sem=send_sem,
        recv_sem=recv_sem,
        device_id=where,
        device_id_type=pl.DeviceIdType.MESH,
    )


def kernel(
    count,
    planes,
    cells,
    vector_part,
    basis,
    coefficients,
    eigen,
    stiffness,
    damping,
    mass,
    used,
    lower,
    upper,
    eig_out,
    res_out,
    norm_out,
    own_basis,
    mate_basis,
    wire_out,
    wire_in,
    values,
    face_out,
    face_in,
    links_in,
    link_sums,
    link_part,
    stat_out,
    stat_in,
    links,
    factors,
    local_sem,
    mate_send,
    mate_recv,
    wire_send,
    wire_recv,
    face_send,
    face_recv,
    stat_send,
    stat_recv,
):
    row = lax.axis_index("rows")
    vec = lax.axis_index("vecs")
    mate = {"vecs": vec + 1 - 2 * (vec % 2)}
    across = {"vecs": (vec + 2) % 4}
    above = {"rows": (row + 1) % count}
    below = {"rows": (row + count - 1) % count}
    half = cells // 2
    eighth = cells // 8
    slots = links.shape[1]
    rank_part = basis.shape[0]

    def plane_at(step):
        return (step + planes - 1) % planes

    def lanes_of(plane):
        return pl.ds(pl.multiple_of(plane * cells, cells), cells)

    def local_copy(plane):
        return pltpu.make_async_copy(
            basis.at[:, lanes_of(plane)], own_basis.at[:, lanes_of(plane)], local_sem.at[plane]
        )

    def mate_copy(plane):
        return remote(
            basis.at[:, lanes_of(plane)],
            mate_basis.at[:, lanes_of(plane)],
            mate_send.at[plane],
            mate_recv.at[plane],
            mate,
        )

    def wire_copy(plane):
        return remote(
            wire_out.at[plane], wire_in.at[plane], wire_send.at[plane], wire_recv.at[plane], across
        )

    def face_copy(which):
        return remote(
            face_out.at[which],
            face_in.at[which],
            face_send.at[which],
            face_recv.at[which],
            above if which == 0 else below,
        )

    def links_copy():
        return remote(links, links_in, face_send.at[2], face_recv.at[2], above)

    def stat_copy(step):
        return remote(
            stat_out,
            stat_in.at[step],
            stat_send.at[step],
            stat_recv.at[step],
            {"rows": (row + step) % count},
        )

    def each(first, last, body):
        def run(step, carry):
            body(step)
            return carry

        lax.fori_loop(first, last, run, 0)

    each(0, planes, lambda step: local_copy(plane_at(step)).start())

    barrier = pltpu.get_barrier_semaphore()

    def greet(where):
        pl.semaphore_signal(barrier, inc=1, device_id=where, device_id_type=pl.DeviceIdType.MESH)

    greet(mate)
    greet(across)
    each(1, count, lambda step: greet({"rows": (row + step) % count}))

    slot = lax.broadcasted_iota(jnp.int32, (1, slots), 1)
    is_used = slot < used[0]
    links[...] = jnp.full_like(links, -1)
    links[0:1] = jnp.where(is_used, lower[...], -1)
    links[1:2] = jnp.where(is_used, upper[...], -1)

    total_vectors, total_rank = coefficients.shape
    place = lax.broadcasted_iota(jnp.int32, (2 * PAD, total_vectors), 0)
    vector = lax.broadcasted_iota(jnp.int32, (2 * PAD, total_vectors), 1)
    owner = jnp.where(place < PAD, vec, (vec + 2) % 4)
    inside = place % PAD
    choose = (inside < vector_part) & (vector == owner * vector_part + inside)
    choose = jnp.where(choose, 1.0, 0.0).astype(jnp.bfloat16)
    chosen = jnp.dot(choose, coefficients[...], preferred_element_type=jnp.float32)
    chosen = chosen.astype(jnp.bfloat16)
    rank = lax.broadcasted_iota(jnp.int32, (total_rank, rank_part), 0)
    own_rank = lax.broadcasted_iota(jnp.int32, (total_rank, rank_part), 1)
    for side, source in enumerate((vec, vec + 1 - 2 * (vec % 2))):
        pick = jnp.where(rank == source * rank_part + own_rank, 1.0, 0.0).astype(jnp.bfloat16)
        part = jnp.dot(chosen, pick, preferred_element_type=jnp.float32)
        factors[side] = part.astype(jnp.bfloat16)

    values[...] = jnp.zeros_like(values)
    stat_out[...] = jnp.zeros_like(stat_out)
    pl.semaphore_wait(barrier, count + 1)

    each(0, planes, lambda step: mate_copy(plane_at(step)).start())
    links_copy().start()

    row_iota = lax.broadcasted_iota(jnp.int32, (FULL, eighth), 0)
    rest = row_iota < vector_part - FULL

    def produce(step):
        plane = plane_at(step)
        local_copy(plane).wait()
        mate_copy(plane).wait_recv()
        both = jnp.dot(
            factors[0], own_basis[:, lanes_of(plane)], preferred_element_type=jnp.float32
        ) + jnp.dot(factors[1], mate_basis[:, lanes_of(plane)], preferred_element_type=jnp.float32)
        values[plane + 1, :, LANES : LANES + cells] = both[:PAD]
        top = both[PAD : PAD + FULL]
        tail = both[PAD + FULL :]
        wire_out[plane, :, :half] = jnp.concatenate([top[:, :half], top[:, half:]], axis=0).astype(
            jnp.bfloat16
        )
        packed = []
        for side in range(2):
            total = None
            for part in range(4):
                start = (4 * side + part) * eighth
                piece = tail[:, start : start + eighth]
                if part:
                    piece = pltpu.roll(piece, 2 * part, 0)
                total = piece if total is None else total + piece
            packed.append(total)
        wire_out[plane, :, half:] = jnp.concatenate(packed, axis=0).astype(jnp.bfloat16)
        wire_copy(plane).start()

    each(0, planes, produce)

    def fold(block):
        total = block[:, :LANES]
        for start in range(LANES, block.shape[1], LANES):
            total = total + block[:, start : start + LANES]
        return total

    def finish(plane):
        wire_copy(plane).wait_recv()
        squares = jnp.zeros((PAD, LANES), jnp.float32)
        for part in range(8):
            side = part // 4
            lanes = slice(LANES + part * eighth, LANES + (part + 1) * eighth)
            inner = (part % 4) * eighth
            top = wire_in[plane, :, inner : inner + eighth].astype(jnp.float32)
            top = top[side * FULL : (side + 1) * FULL]
            tail = wire_in[plane, :, half:].astype(jnp.float32)
            tail = tail[side * FULL : (side + 1) * FULL]
            if part % 4:
                tail = pltpu.roll(tail, FULL - 2 * (part % 4), 0)
            tail = jnp.where(rest, tail, 0.0)
            held = values[plane + 1, :, lanes] + jnp.concatenate([top, tail], axis=0)
            rounded = held.astype(jnp.bfloat16)
            exact = rounded.astype(jnp.float32)
            values[plane + 1, :, lanes] = exact
            start = pl.multiple_of(plane * cells + part * eighth, eighth)
            eig_out[:, pl.ds(start, eighth)] = rounded[:vector_part]
            squares = squares + fold(exact * exact)
        stat_out[:PAD] += squares

    diag = lax.broadcasted_iota(jnp.int32, (PAD, vector_part), 0) == lax.broadcasted_iota(
        jnp.int32, (PAD, vector_part), 1
    )
    lam = jnp.where(diag, jnp.broadcast_to(eigen[...], (PAD, vector_part)), 0.0)
    lam = jnp.sum(lam, axis=1, keepdims=True)
    lam_b = jnp.broadcast_to(lam, (PAD, LANES))
    lam_sq = jnp.tile(lam_b * lam_b, (1, BLOCK // LANES))
    lam_b = jnp.tile(lam_b, (1, BLOCK // LANES))
    coupling = lam_sq * 0.1 + lam_b * 0.3 + 1.0
    column = lax.broadcasted_iota(jnp.int32, (PAD, BLOCK), 1) % WID
    wide = BLOCK + 2 * LANES

    def stencil(plane, link):
        squares = jnp.zeros((PAD, LANES), jnp.float32)
        for start in range(0, cells, BLOCK):
            inner = slice(LANES + start, LANES + start + BLOCK)
            around = values[plane + 1, :, start : start + wide]
            mid = around[:, LANES : LANES + BLOCK]

            def moved(amount):
                return pltpu.roll(around, amount % wide, 1)[:, LANES : LANES + BLOCK]

            total = values[plane, :, inner] + values[plane + 2, :, inner]
            total = total + (moved(WID) + moved(-WID))
            total = total + jnp.where(column < WID - 1, moved(-1), 0.0)
            total = total + jnp.where(column > 0, moved(1), 0.0)
            if link is not None:
                total = total + link_sums[link, :, start : start + BLOCK]
            at = pl.ds(pl.multiple_of(plane * cells + start, BLOCK), BLOCK)
            diagonal = lam_sq * mass[:, at] + lam_b * damping[:, at] + stiffness[:, at]
            full = diagonal * mid - coupling * total
            res_out[:, at] = full.astype(jnp.bfloat16)[:vector_part]
            squares = squares + fold(full * full)
        stat_out[PAD:] += squares

    tiles = cells // LANES

    def link_side(which, lists, source_row, target_row):
        stacked = jnp.concatenate(
            [face_in[which, :, t * LANES : (t + 1) * LANES] for t in range(tiles)], axis=0
        )
        link_part[...] = jnp.zeros_like(link_part)
        low_iota = lax.broadcasted_iota(jnp.int32, (LANES, BLOCK), 0)

        def some(step):
            at = pl.ds(pl.multiple_of(step * BLOCK, BLOCK), BLOCK)
            source = lists[source_row : source_row + 1, at]
            target = lists[target_row : target_row + 1, at]
            low = jnp.where(low_iota == (source & (LANES - 1)), 1.0, 0.0).astype(jnp.bfloat16)
            picked = jnp.dot(stacked, low, preferred_element_type=jnp.float32)
            high = jnp.broadcast_to(source >> 7, (PAD, BLOCK))
            got = jnp.zeros((PAD, BLOCK), jnp.float32)
            for t in range(tiles):
                got = got + jnp.where(high == t, picked[t * PAD : (t + 1) * PAD], 0.0)
            high = jnp.broadcast_to(target >> 7, (PAD, BLOCK))
            spread = jnp.concatenate(
                [jnp.where(high == t, got, 0.0).astype(jnp.bfloat16) for t in range(tiles)], axis=0
            )
            low = jnp.where(low_iota == (target & (LANES - 1)), 1.0, 0.0).astype(jnp.bfloat16)
            link_part[...] += lax.dot_general(
                spread, low, (((1,), (1,)), ((), ())), preferred_element_type=jnp.float32
            )

        each(0, slots // BLOCK, some)
        for t in range(tiles):
            link_sums[which, :, t * LANES : (t + 1) * LANES] = link_part[t * PAD : (t + 1) * PAD]

    def send_face(which, plane):
        face_out[which] = values[plane + 1, :, LANES : LANES + cells].astype(jnp.bfloat16)
        face_copy(which).start()

    finish(planes - 1)
    send_face(0, planes - 1)
    finish(0)
    send_face(1, 0)
    finish(1)

    def advance(plane):
        finish(plane)
        stencil(plane - 1, None)

    middle = max(2, planes // 2 - 1)
    each(2, middle, advance)
    face_copy(0).wait_recv()
    links_copy().wait_recv()
    link_side(0, links_in, 0, 1)
    face_copy(1).wait_recv()
    link_side(1, links, 1, 0)
    stencil(0, 0)
    each(middle, planes - 1, advance)
    stencil(planes - 2, None)
    stencil(planes - 1, 1)

    each(1, count, lambda step: stat_copy(step).start())
    stat_in[0] = stat_out[...]
    each(1, count, lambda step: stat_copy(step).wait_recv())
    total = stat_in[0]
    for step in range(1, count):
        total = total + stat_in[step]
    sums = jnp.sum(total, axis=1, keepdims=True)
    norms = jnp.sqrt(sums[PAD:]) / jnp.sqrt(sums[:PAD] + 1.0)
    norms = jnp.where(diag, jnp.broadcast_to(norms, (PAD, vector_part)), 0.0)
    norm_out[...] = jnp.sum(norms, axis=0, keepdims=True)

    each(0, planes, lambda plane: mate_copy(plane).wait_send())
    each(0, planes, lambda plane: wire_copy(plane).wait_send())
    links_copy().wait_send()
    face_copy(0).wait_send()
    face_copy(1).wait_send()
    each(1, count, lambda step: stat_copy(step).wait_send())


def on_device(
    basis,
    coefficients,
    eigen_values,
    stiffness,
    damping,
    mass,
    link_count,
    lower_cells,
    upper_cells,
):
    count = lax.axis_size("rows")
    vector_part = eigen_values.shape[0]
    rank_part, rows_local = basis.shape
    cells = WID * WID
    planes = rows_local // cells
    slots = lower_cells.shape[1]
    vmem = pl.BlockSpec(memory_space=pltpu.VMEM)
    wire = cells // 2 + cells // 8
    dma = pltpu.SemaphoreType.DMA
    eigvecs, residuals, norms = pl.pallas_call(
        functools.partial(kernel, count, planes, cells, vector_part),
        out_shape=(
            jax.ShapeDtypeStruct((vector_part, rows_local), jnp.bfloat16),
            jax.ShapeDtypeStruct((vector_part, rows_local), jnp.bfloat16),
            jax.ShapeDtypeStruct((1, vector_part), jnp.float32),
        ),
        in_specs=[pl.BlockSpec(memory_space=pl.ANY)] + [vmem] * 5 + [pl.BlockSpec(memory_space=pltpu.SMEM), vmem, vmem],
        out_specs=(vmem, vmem, vmem),
        scratch_shapes=[
            pltpu.VMEM((rank_part, rows_local), jnp.bfloat16),
            pltpu.VMEM((rank_part, rows_local), jnp.bfloat16),
            pltpu.VMEM((planes, PAD, wire), jnp.bfloat16),
            pltpu.VMEM((planes, PAD, wire), jnp.bfloat16),
            pltpu.VMEM((planes + 2, PAD, cells + 2 * LANES), jnp.float32),
            pltpu.VMEM((2, PAD, cells), jnp.bfloat16),
            pltpu.VMEM((2, PAD, cells), jnp.bfloat16),
            pltpu.VMEM((8, slots), jnp.int32),
            pltpu.VMEM((2, PAD, cells), jnp.float32),
            pltpu.VMEM((cells // LANES * PAD, LANES), jnp.float32),
            pltpu.VMEM((2 * PAD, LANES), jnp.float32),
            pltpu.VMEM((count, 2 * PAD, LANES), jnp.float32),
            pltpu.VMEM((8, slots), jnp.int32),
            pltpu.VMEM((2, 2 * PAD, rank_part), jnp.bfloat16),
            dma((planes,)),
            dma((planes,)),
            dma((planes,)),
            dma((planes,)),
            dma((planes,)),
            dma((3,)),
            dma((3,)),
            dma((count,)),
            dma((count,)),
        ],
        compiler_params=pltpu.CompilerParams(
            collective_id=0, has_side_effects=True, vmem_limit_bytes=56 * 1024 * 1024
        ),
    )(
        basis,
        coefficients.T,
        eigen_values[None, :],
        stiffness[None, :],
        damping[None, :],
        mass[None, :],
        link_count,
        lower_cells,
        upper_cells,
    )
    return eigvecs, residuals, norms[0]


def solution(mesh):
    placed = (
        P("vecs", "rows"),
        P(),
        P("vecs"),
        P("rows"),
        P("rows"),
        P("rows"),
        P("rows"),
        P("rows", None),
        P("rows", None),
    )
    return jax.shard_map(
        on_device,
        mesh=mesh,
        in_specs=placed,
        out_specs=(P("vecs", "rows"), P("vecs", "rows"), P("vecs")),
        check_vma=False,
    )
```

```python
import functools

import jax
import jax.numpy as jnp
from jax import lax
from jax.experimental import pallas as pl
from jax.experimental.pallas import tpu as pltpu
from jax.sharding import PartitionSpec as P

WID = 64
LANES = 128
PAD = 16
BLOCK = 512
FULL = 8


def remote(src, dst, send_sem, recv_sem, where):
    return pltpu.make_async_remote_copy(
        src_ref=src,
        dst_ref=dst,
        send_sem=send_sem,
        recv_sem=recv_sem,
        device_id=where,
        device_id_type=pl.DeviceIdType.MESH,
    )


def kernel(
    count,
    planes,
    cells,
    vector_part,
    basis,
    coefficients,
    eigen,
    stiffness_in,
    damping_in,
    mass_in,
    used,
    lower,
    upper,
    eig_out,
    res_out,
    norm_out,
    own_basis,
    mate_basis,
    wire_out,
    wire_in,
    values,
    face_out,
    face_in,
    links_in,
    link_sums,
    link_part,
    stat_out,
    stat_in,
    links,
    factors,
    stiffness,
    damping,
    mass,
    stat_line,
    input_sem,
    local_sem,
    mate_send,
    mate_recv,
    wire_send,
    wire_recv,
    face_send,
    face_recv,
    stat_send,
    stat_recv,
):
    row = lax.axis_index("rows")
    vec = lax.axis_index("vecs")
    mate = {"vecs": vec + 1 - 2 * (vec % 2)}
    across = {"vecs": (vec + 2) % 4}
    above = {"rows": (row + 1) % count}
    below = {"rows": (row + count - 1) % count}
    half = cells // 2
    eighth = cells // 8
    slots = links.shape[1]
    rank_part = basis.shape[0]

    def plane_at(step):
        return (step + planes - 1) % planes

    def lanes_of(plane):
        return pl.ds(pl.multiple_of(plane * cells, cells), cells)

    def local_copy(plane):
        return pltpu.make_async_copy(
            basis.at[:, lanes_of(plane)], own_basis.at[:, lanes_of(plane)], local_sem.at[plane]
        )

    def mate_copy(plane):
        return remote(
            basis.at[:, lanes_of(plane)],
            mate_basis.at[:, lanes_of(plane)],
            mate_send.at[plane],
            mate_recv.at[plane],
            mate,
        )

    def wire_copy(plane):
        return remote(
            wire_out.at[plane], wire_in.at[plane], wire_send.at[plane], wire_recv.at[plane], across
        )

    def face_copy(which):
        return remote(
            face_out.at[which],
            face_in.at[which],
            face_send.at[which],
            face_recv.at[which],
            above if which == 0 else below,
        )

    def links_copy():
        return remote(links, links_in, face_send.at[2], face_recv.at[2], above)

    def stat_copy(step):
        return remote(
            stat_line,
            stat_in.at[step],
            stat_send.at[step],
            stat_recv.at[step],
            {"rows": (row + step) % count},
        )

    def each(first, last, body):
        def run(step, carry):
            body(step)
            return carry

        lax.fori_loop(first, last, run, 0)

    each(0, planes, lambda step: local_copy(plane_at(step)).start())
    diagonals = [
        pltpu.make_async_copy(source, target, input_sem.at[place])
        for place, (source, target) in enumerate(
            ((stiffness_in, stiffness), (damping_in, damping), (mass_in, mass))
        )
    ]
    for copy in diagonals:
        copy.start()

    barrier = pltpu.get_barrier_semaphore()

    def greet(where):
        pl.semaphore_signal(barrier, inc=1, device_id=where, device_id_type=pl.DeviceIdType.MESH)

    greet(mate)
    greet(across)
    each(1, count, lambda step: greet({"rows": (row + step) % count}))

    slot = lax.broadcasted_iota(jnp.int32, (1, slots), 1)
    is_used = slot < used[0]
    links[...] = jnp.full_like(links, -1)
    links[0:1] = jnp.where(is_used, lower[...], -1)
    links[1:2] = jnp.where(is_used, upper[...], -1)

    total_vectors, total_rank = coefficients.shape
    place = lax.broadcasted_iota(jnp.int32, (2 * PAD, total_vectors), 0)
    vector = lax.broadcasted_iota(jnp.int32, (2 * PAD, total_vectors), 1)
    owner = jnp.where(place < PAD, vec, (vec + 2) % 4)
    inside = place % PAD
    choose = (inside < vector_part) & (vector == owner * vector_part + inside)
    choose = jnp.where(choose, 1.0, 0.0).astype(jnp.bfloat16)
    chosen = jnp.dot(choose, coefficients[...], preferred_element_type=jnp.float32)
    chosen = chosen.astype(jnp.bfloat16)
    rank = lax.broadcasted_iota(jnp.int32, (total_rank, rank_part), 0)
    own_rank = lax.broadcasted_iota(jnp.int32, (total_rank, rank_part), 1)
    for side, source in enumerate((vec, vec + 1 - 2 * (vec % 2))):
        pick = jnp.where(rank == source * rank_part + own_rank, 1.0, 0.0).astype(jnp.bfloat16)
        part = jnp.dot(chosen, pick, preferred_element_type=jnp.float32)
        factors[side] = part.astype(jnp.bfloat16)

    values[...] = jnp.zeros_like(values)
    stat_out[...] = jnp.zeros_like(stat_out)
    pl.semaphore_wait(barrier, count + 1)

    each(0, planes, lambda step: mate_copy(plane_at(step)).start())
    links_copy().start()

    row_iota = lax.broadcasted_iota(jnp.int32, (FULL, eighth), 0)
    rest = row_iota < vector_part - FULL

    def produce(step):
        plane = plane_at(step)
        local_copy(plane).wait()
        mate_copy(plane).wait_recv()
        both = jnp.dot(
            factors[0], own_basis[:, lanes_of(plane)], preferred_element_type=jnp.float32
        ) + jnp.dot(factors[1], mate_basis[:, lanes_of(plane)], preferred_element_type=jnp.float32)
        values[plane + 1, :, LANES : LANES + cells] = both[:PAD]
        top = both[PAD : PAD + FULL]
        tail = both[PAD + FULL :]
        wire_out[plane, :, :half] = jnp.concatenate([top[:, :half], top[:, half:]], axis=0).astype(
            jnp.bfloat16
        )
        packed = []
        for side in range(2):
            total = None
            for part in range(4):
                start = (4 * side + part) * eighth
                piece = tail[:, start : start + eighth]
                if part:
                    piece = pltpu.roll(piece, 2 * part, 0)
                total = piece if total is None else total + piece
            packed.append(total)
        wire_out[plane, :, half:] = jnp.concatenate(packed, axis=0).astype(jnp.bfloat16)
        wire_copy(plane).start()

    each(0, planes, produce)
    for copy in diagonals:
        copy.wait()

    def fold(block):
        total = block[:, :LANES]
        for start in range(LANES, block.shape[1], LANES):
            total = total + block[:, start : start + LANES]
        return total

    def finish(plane):
        wire_copy(plane).wait_recv()
        squares = jnp.zeros((PAD, LANES), jnp.float32)
        for part in range(8):
            side = part // 4
            lanes = slice(LANES + part * eighth, LANES + (part + 1) * eighth)
            inner = (part % 4) * eighth
            top = wire_in[plane, :, inner : inner + eighth].astype(jnp.float32)
            top = top[side * FULL : (side + 1) * FULL]
            tail = wire_in[plane, :, half:].astype(jnp.float32)
            tail = tail[side * FULL : (side + 1) * FULL]
            if part % 4:
                tail = pltpu.roll(tail, FULL - 2 * (part % 4), 0)
            tail = jnp.where(rest, tail, 0.0)
            held = values[plane + 1, :, lanes] + jnp.concatenate([top, tail], axis=0)
            rounded = held.astype(jnp.bfloat16)
            exact = rounded.astype(jnp.float32)
            values[plane + 1, :, lanes] = exact
            start = pl.multiple_of(plane * cells + part * eighth, eighth)
            eig_out[:, pl.ds(start, eighth)] = rounded[:vector_part]
            squares = squares + fold(exact * exact)
        stat_out[:PAD] += squares

    diag = lax.broadcasted_iota(jnp.int32, (PAD, vector_part), 0) == lax.broadcasted_iota(
        jnp.int32, (PAD, vector_part), 1
    )
    lam = jnp.where(diag, jnp.broadcast_to(eigen[...], (PAD, vector_part)), 0.0)
    lam = jnp.sum(lam, axis=1, keepdims=True)
    lam_b = jnp.broadcast_to(lam, (PAD, LANES))
    lam_sq = jnp.tile(lam_b * lam_b, (1, BLOCK // LANES))
    lam_b = jnp.tile(lam_b, (1, BLOCK // LANES))
    coupling = lam_sq * 0.1 + lam_b * 0.3 + 1.0
    column = lax.broadcasted_iota(jnp.int32, (PAD, BLOCK), 1) % WID
    wide = BLOCK + 2 * LANES

    def stencil(plane, link):
        squares = jnp.zeros((PAD, LANES), jnp.float32)
        for start in range(0, cells, BLOCK):
            inner = slice(LANES + start, LANES + start + BLOCK)
            around = values[plane + 1, :, start : start + wide]
            mid = around[:, LANES : LANES + BLOCK]

            def moved(amount):
                return pltpu.roll(around, amount % wide, 1)[:, LANES : LANES + BLOCK]

            total = values[plane, :, inner] + values[plane + 2, :, inner]
            total = total + (moved(WID) + moved(-WID))
            total = total + jnp.where(column < WID - 1, moved(-1), 0.0)
            total = total + jnp.where(column > 0, moved(1), 0.0)
            if link is not None:
                total = total + link_sums[link, :, start : start + BLOCK]
            at = pl.ds(pl.multiple_of(plane * cells + start, BLOCK), BLOCK)
            diagonal = lam_sq * mass[:, at] + lam_b * damping[:, at] + stiffness[:, at]
            full = diagonal * mid - coupling * total
            res_out[:, at] = full.astype(jnp.bfloat16)[:vector_part]
            squares = squares + fold(full * full)
        stat_out[PAD:] += squares

    tiles = cells // LANES

    def link_side(which, lists, source_row, target_row):
        stacked = jnp.concatenate(
            [face_in[which, :, t * LANES : (t + 1) * LANES] for t in range(tiles)], axis=0
        )
        link_part[...] = jnp.zeros_like(link_part)
        low_iota = lax.broadcasted_iota(jnp.int32, (LANES, BLOCK), 0)

        def some(step):
            at = pl.ds(pl.multiple_of(step * BLOCK, BLOCK), BLOCK)
            source = lists[source_row : source_row + 1, at]
            target = lists[target_row : target_row + 1, at]
            low = jnp.where(low_iota == (source & (LANES - 1)), 1.0, 0.0).astype(jnp.bfloat16)
            picked = jnp.dot(stacked, low, preferred_element_type=jnp.float32)
            high = jnp.broadcast_to(source >> 7, (PAD, BLOCK))
            got = jnp.zeros((PAD, BLOCK), jnp.float32)
            for t in range(tiles):
                got = got + jnp.where(high == t, picked[t * PAD : (t + 1) * PAD], 0.0)
            high = jnp.broadcast_to(target >> 7, (PAD, BLOCK))
            spread = jnp.concatenate(
                [jnp.where(high == t, got, 0.0).astype(jnp.bfloat16) for t in range(tiles)], axis=0
            )
            low = jnp.where(low_iota == (target & (LANES - 1)), 1.0, 0.0).astype(jnp.bfloat16)
            link_part[...] += lax.dot_general(
                spread, low, (((1,), (1,)), ((), ())), preferred_element_type=jnp.float32
            )

        each(0, slots // BLOCK, some)
        for t in range(tiles):
            link_sums[which, :, t * LANES : (t + 1) * LANES] = link_part[t * PAD : (t + 1) * PAD]

    def send_face(which, plane):
        face_out[which] = values[plane + 1, :, LANES : LANES + cells].astype(jnp.bfloat16)
        face_copy(which).start()

    finish(planes - 1)
    send_face(0, planes - 1)
    finish(0)
    send_face(1, 0)
    finish(1)

    def advance(plane):
        finish(plane)
        stencil(plane - 1, None)

    middle = min(4, planes - 1)
    each(2, middle, advance)
    face_copy(0).wait_recv()
    links_copy().wait_recv()
    link_side(0, links_in, 0, 1)
    face_copy(1).wait_recv()
    link_side(1, links, 1, 0)
    stencil(0, 0)
    each(middle, planes - 1, advance)
    stencil(planes - 2, None)
    stencil(planes - 1, 1)

    sums = jnp.sum(stat_out[...], axis=1, keepdims=True)
    spot = lax.broadcasted_iota(jnp.int32, (2 * PAD, LANES), 0) == lax.broadcasted_iota(
        jnp.int32, (2 * PAD, LANES), 1
    )
    line = jnp.sum(jnp.where(spot, sums, 0.0), axis=0, keepdims=True)
    stat_line[...] = line
    each(1, count, lambda step: stat_copy(step).start())
    each(0, planes, lambda plane: mate_copy(plane).wait_send())
    each(0, planes, lambda plane: wire_copy(plane).wait_send())
    links_copy().wait_send()
    face_copy(0).wait_send()
    face_copy(1).wait_send()
    each(1, count, lambda step: stat_copy(step).wait_recv())
    for step in range(1, count):
        line = line + stat_in[step]
    norms = jnp.sqrt(line[:, PAD : PAD + vector_part]) / jnp.sqrt(line[:, :vector_part] + 1.0)
    norm_out[...] = norms
    each(1, count, lambda step: stat_copy(step).wait_send())


def on_device(
    basis,
    coefficients,
    eigen_values,
    stiffness,
    damping,
    mass,
    link_count,
    lower_cells,
    upper_cells,
):
    count = lax.axis_size("rows")
    vector_part = eigen_values.shape[0]
    rank_part, rows_local = basis.shape
    cells = WID * WID
    planes = rows_local // cells
    slots = lower_cells.shape[1]
    vmem = pl.BlockSpec(memory_space=pltpu.VMEM)
    anywhere = pl.BlockSpec(memory_space=pltpu.HBM)
    wire = cells // 2 + cells // 8
    dma = pltpu.SemaphoreType.DMA
    eigvecs, residuals, norms = pl.pallas_call(
        functools.partial(kernel, count, planes, cells, vector_part),
        out_shape=(
            pltpu.VMEM((vector_part, rows_local), jnp.bfloat16),
            pltpu.VMEM((vector_part, rows_local), jnp.bfloat16),
            jax.ShapeDtypeStruct((1, vector_part), jnp.float32),
        ),
        in_specs=[anywhere, vmem, vmem, anywhere, anywhere, anywhere] + [pl.BlockSpec(memory_space=pltpu.SMEM), vmem, vmem],
        out_specs=(vmem, vmem, vmem),
        scratch_shapes=[
            pltpu.VMEM((rank_part, rows_local), jnp.bfloat16),
            pltpu.VMEM((rank_part, rows_local), jnp.bfloat16),
            pltpu.VMEM((planes, PAD, wire), jnp.bfloat16),
            pltpu.VMEM((planes, PAD, wire), jnp.bfloat16),
            pltpu.VMEM((planes + 2, PAD, cells + 2 * LANES), jnp.float32),
            pltpu.VMEM((2, PAD, cells), jnp.bfloat16),
            pltpu.VMEM((2, PAD, cells), jnp.bfloat16),
            pltpu.VMEM((8, slots), jnp.int32),
            pltpu.VMEM((2, PAD, cells), jnp.float32),
            pltpu.VMEM((cells // LANES * PAD, LANES), jnp.float32),
            pltpu.VMEM((2 * PAD, LANES), jnp.float32),
            pltpu.VMEM((count, 1, LANES), jnp.float32),
            pltpu.VMEM((8, slots), jnp.int32),
            pltpu.VMEM((2, 2 * PAD, rank_part), jnp.bfloat16),
            pltpu.VMEM((1, rows_local), jnp.float32),
            pltpu.VMEM((1, rows_local), jnp.float32),
            pltpu.VMEM((1, rows_local), jnp.float32),
            pltpu.VMEM((1, LANES), jnp.float32),
            dma((3,)),
            dma((planes,)),
            dma((planes,)),
            dma((planes,)),
            dma((planes,)),
            dma((planes,)),
            dma((3,)),
            dma((3,)),
            dma((count,)),
            dma((count,)),
        ],
        compiler_params=pltpu.CompilerParams(
            collective_id=0, has_side_effects=True, vmem_limit_bytes=56 * 1024 * 1024
        ),
    )(
        basis,
        coefficients.T,
        eigen_values[None, :],
        stiffness[None, :],
        damping[None, :],
        mass[None, :],
        link_count,
        lower_cells,
        upper_cells,
    )
    return eigvecs, residuals, norms[0]


def solution(mesh):
    placed = (
        P("vecs", "rows"),
        P(),
        P("vecs"),
        P("rows"),
        P("rows"),
        P("rows"),
        P("rows"),
        P("rows", None),
        P("rows", None),
    )
    return jax.shard_map(
        on_device,
        mesh=mesh,
        in_specs=placed,
        out_specs=(P("vecs", "rows"), P("vecs", "rows"), P("vecs")),
        check_vma=False,
    )
```

```python
import functools

import jax
import jax.numpy as jnp
from jax import lax
from jax.experimental import pallas as pl
from jax.experimental.pallas import tpu as pltpu
from jax.sharding import PartitionSpec as P

WID = 64
LANES = 128
PAD = 16
BLOCK = 512
FULL = 8


def remote(src, dst, send_sem, recv_sem, where):
    return pltpu.make_async_remote_copy(
        src_ref=src,
        dst_ref=dst,
        send_sem=send_sem,
        recv_sem=recv_sem,
        device_id=where,
        device_id_type=pl.DeviceIdType.MESH,
    )


def kernel(
    count,
    planes,
    cells,
    vector_part,
    basis,
    coefficients_in,
    eigen_in,
    stiffness_in,
    damping_in,
    mass_in,
    used_in,
    lower_in,
    upper_in,
    eig_out,
    res_out,
    norm_out,
    own_basis,
    mate_basis,
    wire_out,
    wire_in,
    values,
    face_out,
    face_in,
    links_in,
    link_sums,
    link_part,
    stat_out,
    stat_in,
    links,
    factors,
    stiffness,
    damping,
    mass,
    stat_line,
    coefficients,
    eigen,
    used,
    lower,
    upper,
    input_sem,
    local_sem,
    mate_send,
    mate_recv,
    wire_send,
    wire_recv,
    face_send,
    face_recv,
    stat_send,
    stat_recv,
):
    row = lax.axis_index("rows")
    vec = lax.axis_index("vecs")
    mate = {"vecs": vec + 1 - 2 * (vec % 2)}
    across = {"vecs": (vec + 2) % 4}
    above = {"rows": (row + 1) % count}
    below = {"rows": (row + count - 1) % count}
    half = cells // 2
    eighth = cells // 8
    slots = links.shape[1]
    rank_part = basis.shape[0]

    def plane_at(step):
        return (step + planes - 1) % planes

    def lanes_of(plane):
        return pl.ds(pl.multiple_of(plane * cells, cells), cells)

    def local_copy(plane):
        return pltpu.make_async_copy(
            basis.at[:, lanes_of(plane)], own_basis.at[:, lanes_of(plane)], local_sem.at[plane]
        )

    def mate_copy(plane):
        return remote(
            own_basis.at[:, lanes_of(plane)],
            mate_basis.at[:, lanes_of(plane)],
            mate_send.at[plane],
            mate_recv.at[plane],
            mate,
        )

    def wire_copy(plane):
        return remote(
            wire_out.at[plane], wire_in.at[plane], wire_send.at[plane], wire_recv.at[plane], across
        )

    def face_copy(which):
        return remote(
            face_out.at[which],
            face_in.at[which],
            face_send.at[which],
            face_recv.at[which],
            above if which == 0 else below,
        )

    def links_copy():
        return remote(links, links_in, face_send.at[2], face_recv.at[2], above)

    def stat_copy(step):
        return remote(
            stat_line,
            stat_in.at[step],
            stat_send.at[step],
            stat_recv.at[step],
            {"rows": (row + step) % count},
        )

    def each(first, last, body):
        def run(step, carry):
            body(step)
            return carry

        lax.fori_loop(first, last, run, 0)

    barrier = pltpu.get_barrier_semaphore()

    def greet(where):
        pl.semaphore_signal(barrier, inc=1, device_id=where, device_id_type=pl.DeviceIdType.MESH)

    each(1, count, lambda step: greet({"rows": (row + step) % count}))
    greet(mate)
    greet(across)

    inputs = [
        pltpu.make_async_copy(source, target, input_sem.at[place])
        for place, (source, target) in enumerate(
            (
                (coefficients_in, coefficients),
                (eigen_in, eigen),
                (used_in, used),
                (lower_in, lower),
                (upper_in, upper),
                (stiffness_in, stiffness),
                (damping_in, damping),
                (mass_in, mass),
            )
        )
    ]
    for copy in inputs[:5]:
        copy.start()
    each(0, planes, lambda step: local_copy(plane_at(step)).start())
    for copy in inputs[5:]:
        copy.start()

    values[...] = jnp.zeros_like(values)
    stat_out[...] = jnp.zeros_like(stat_out)
    for copy in inputs[:5]:
        copy.wait()

    slot = lax.broadcasted_iota(jnp.int32, (1, slots), 1)
    is_used = slot < used[0]
    links[...] = jnp.full_like(links, -1)
    links[0:1] = jnp.where(is_used, lower[...], -1)
    links[1:2] = jnp.where(is_used, upper[...], -1)

    total_vectors, total_rank = coefficients.shape
    place = lax.broadcasted_iota(jnp.int32, (2 * PAD, total_vectors), 0)
    vector = lax.broadcasted_iota(jnp.int32, (2 * PAD, total_vectors), 1)
    owner = jnp.where(place < PAD, vec, (vec + 2) % 4)
    inside = place % PAD
    choose = (inside < vector_part) & (vector == owner * vector_part + inside)
    choose = jnp.where(choose, 1.0, 0.0).astype(jnp.bfloat16)
    chosen = jnp.dot(choose, coefficients[...], preferred_element_type=jnp.float32)
    chosen = chosen.astype(jnp.bfloat16)
    rank = lax.broadcasted_iota(jnp.int32, (total_rank, rank_part), 0)
    own_rank = lax.broadcasted_iota(jnp.int32, (total_rank, rank_part), 1)
    for side, source in enumerate((vec, vec + 1 - 2 * (vec % 2))):
        pick = jnp.where(rank == source * rank_part + own_rank, 1.0, 0.0).astype(jnp.bfloat16)
        part = jnp.dot(chosen, pick, preferred_element_type=jnp.float32)
        factors[side] = part.astype(jnp.bfloat16)

    pl.semaphore_wait(barrier, count + 1)

    def pass_on(step):
        local_copy(plane_at(step)).wait()
        mate_copy(plane_at(step)).start()

    each(0, planes, pass_on)
    links_copy().start()

    row_iota = lax.broadcasted_iota(jnp.int32, (FULL, eighth), 0)
    rest = row_iota < vector_part - FULL

    def produce(step):
        plane = plane_at(step)
        mate_copy(plane).wait_recv()
        both = jnp.dot(
            factors[0], own_basis[:, lanes_of(plane)], preferred_element_type=jnp.float32
        ) + jnp.dot(factors[1], mate_basis[:, lanes_of(plane)], preferred_element_type=jnp.float32)
        values[plane + 1, :, LANES : LANES + cells] = both[:PAD]
        top = both[PAD : PAD + FULL]
        tail = both[PAD + FULL :]
        wire_out[plane, :, :half] = jnp.concatenate([top[:, :half], top[:, half:]], axis=0).astype(
            jnp.bfloat16
        )
        packed = []
        for side in range(2):
            total = None
            for part in range(4):
                start = (4 * side + part) * eighth
                piece = tail[:, start : start + eighth]
                if part:
                    piece = pltpu.roll(piece, 2 * part, 0)
                total = piece if total is None else total + piece
            packed.append(total)
        wire_out[plane, :, half:] = jnp.concatenate(packed, axis=0).astype(jnp.bfloat16)
        wire_copy(plane).start()

    each(0, planes, produce)
    for copy in inputs[5:]:
        copy.wait()

    def fold(block):
        total = block[:, :LANES]
        for start in range(LANES, block.shape[1], LANES):
            total = total + block[:, start : start + LANES]
        return total

    def finish(plane):
        wire_copy(plane).wait_recv()
        squares = jnp.zeros((PAD, LANES), jnp.float32)
        for part in range(8):
            side = part // 4
            lanes = slice(LANES + part * eighth, LANES + (part + 1) * eighth)
            inner = (part % 4) * eighth
            top = wire_in[plane, :, inner : inner + eighth].astype(jnp.float32)
            top = top[side * FULL : (side + 1) * FULL]
            tail = wire_in[plane, :, half:].astype(jnp.float32)
            tail = tail[side * FULL : (side + 1) * FULL]
            if part % 4:
                tail = pltpu.roll(tail, FULL - 2 * (part % 4), 0)
            tail = jnp.where(rest, tail, 0.0)
            held = values[plane + 1, :, lanes] + jnp.concatenate([top, tail], axis=0)
            rounded = held.astype(jnp.bfloat16)
            exact = rounded.astype(jnp.float32)
            values[plane + 1, :, lanes] = exact
            start = pl.multiple_of(plane * cells + part * eighth, eighth)
            eig_out[:, pl.ds(start, eighth)] = rounded[:vector_part]
            squares = squares + fold(exact * exact)
        stat_out[:PAD] += squares

    diag = lax.broadcasted_iota(jnp.int32, (PAD, vector_part), 0) == lax.broadcasted_iota(
        jnp.int32, (PAD, vector_part), 1
    )
    lam = jnp.where(diag, jnp.broadcast_to(eigen[...], (PAD, vector_part)), 0.0)
    lam = jnp.sum(lam, axis=1, keepdims=True)
    lam_b = jnp.broadcast_to(lam, (PAD, LANES))
    lam_sq = jnp.tile(lam_b * lam_b, (1, BLOCK // LANES))
    lam_b = jnp.tile(lam_b, (1, BLOCK // LANES))
    coupling = lam_sq * 0.1 + lam_b * 0.3 + 1.0
    column = lax.broadcasted_iota(jnp.int32, (PAD, BLOCK), 1) % WID
    wide = BLOCK + 2 * LANES

    def stencil(plane, link):
        squares = jnp.zeros((PAD, LANES), jnp.float32)
        for start in range(0, cells, BLOCK):
            inner = slice(LANES + start, LANES + start + BLOCK)
            around = values[plane + 1, :, start : start + wide]
            mid = around[:, LANES : LANES + BLOCK]

            def moved(amount):
                return pltpu.roll(around, amount % wide, 1)[:, LANES : LANES + BLOCK]

            total = values[plane, :, inner] + values[plane + 2, :, inner]
            total = total + (moved(WID) + moved(-WID))
            total = total + jnp.where(column < WID - 1, moved(-1), 0.0)
            total = total + jnp.where(column > 0, moved(1), 0.0)
            if link is not None:
                total = total + link_sums[link, :, start : start + BLOCK]
            at = pl.ds(pl.multiple_of(plane * cells + start, BLOCK), BLOCK)
            diagonal = lam_sq * mass[:, at] + lam_b * damping[:, at] + stiffness[:, at]
            full = diagonal * mid - coupling * total
            res_out[:, at] = full.astype(jnp.bfloat16)[:vector_part]
            squares = squares + fold(full * full)
        stat_out[PAD:] += squares

    tiles = cells // LANES

    def link_side(which, lists, source_row, target_row):
        stacked = jnp.concatenate(
            [face_in[which, :, t * LANES : (t + 1) * LANES] for t in range(tiles)], axis=0
        )
        link_part[...] = jnp.zeros_like(link_part)
        low_iota = lax.broadcasted_iota(jnp.int32, (LANES, BLOCK), 0)

        def some(step):
            at = pl.ds(pl.multiple_of(step * BLOCK, BLOCK), BLOCK)
            source = lists[source_row : source_row + 1, at]
            target = lists[target_row : target_row + 1, at]
            low = jnp.where(low_iota == (source & (LANES - 1)), 1.0, 0.0).astype(jnp.bfloat16)
            picked = jnp.dot(stacked, low, preferred_element_type=jnp.float32)
            high = jnp.broadcast_to(source >> 7, (PAD, BLOCK))
            got = jnp.zeros((PAD, BLOCK), jnp.float32)
            for t in range(tiles):
                got = got + jnp.where(high == t, picked[t * PAD : (t + 1) * PAD], 0.0)
            high = jnp.broadcast_to(target >> 7, (PAD, BLOCK))
            spread = jnp.concatenate(
                [jnp.where(high == t, got, 0.0).astype(jnp.bfloat16) for t in range(tiles)], axis=0
            )
            low = jnp.where(low_iota == (target & (LANES - 1)), 1.0, 0.0).astype(jnp.bfloat16)
            link_part[...] += lax.dot_general(
                spread, low, (((1,), (1,)), ((), ())), preferred_element_type=jnp.float32
            )

        each(0, slots // BLOCK, some)
        for t in range(tiles):
            link_sums[which, :, t * LANES : (t + 1) * LANES] = link_part[t * PAD : (t + 1) * PAD]

    def send_face(which, plane):
        face_out[which] = values[plane + 1, :, LANES : LANES + cells].astype(jnp.bfloat16)
        face_copy(which).start()

    finish(planes - 1)
    send_face(0, planes - 1)
    finish(0)
    send_face(1, 0)
    finish(1)

    def advance(plane):
        finish(plane)
        stencil(plane - 1, None)

    middle = min(4, planes - 1)
    each(2, middle, advance)
    face_copy(0).wait_recv()
    links_copy().wait_recv()
    link_side(0, links_in, 0, 1)
    face_copy(1).wait_recv()
    link_side(1, links, 1, 0)
    stencil(0, 0)
    each(middle, planes - 1, advance)
    stencil(planes - 2, None)
    stencil(planes - 1, 1)

    sums = jnp.sum(stat_out[...], axis=1, keepdims=True)
    spot = lax.broadcasted_iota(jnp.int32, (2 * PAD, LANES), 0) == lax.broadcasted_iota(
        jnp.int32, (2 * PAD, LANES), 1
    )
    line = jnp.sum(jnp.where(spot, sums, 0.0), axis=0, keepdims=True)
    stat_line[...] = line
    each(1, count, lambda step: stat_copy(step).start())
    each(0, planes, lambda plane: mate_copy(plane).wait_send())
    each(0, planes, lambda plane: wire_copy(plane).wait_send())
    links_copy().wait_send()
    face_copy(0).wait_send()
    face_copy(1).wait_send()
    each(1, count, lambda step: stat_copy(step).wait_recv())
    for step in range(1, count):
        line = line + stat_in[step]
    norms = jnp.sqrt(line[:, PAD : PAD + vector_part]) / jnp.sqrt(line[:, :vector_part] + 1.0)
    norm_out[...] = norms
    each(1, count, lambda step: stat_copy(step).wait_send())


def write_back(eig_held, res_held, norm_held, eig_out, res_out, norm_out, sem):
    copies = [
        pltpu.make_async_copy(source, target, sem.at[place])
        for place, (source, target) in enumerate(
            ((eig_held, eig_out), (res_held, res_out), (norm_held, norm_out))
        )
    ]
    for copy in copies:
        copy.start()
    for copy in copies:
        copy.wait()


def on_device(
    basis,
    coefficients,
    eigen_values,
    stiffness,
    damping,
    mass,
    link_count,
    lower_cells,
    upper_cells,
):
    count = lax.axis_size("rows")
    vector_part = eigen_values.shape[0]
    rank_part, rows_local = basis.shape
    cells = WID * WID
    planes = rows_local // cells
    slots = lower_cells.shape[1]
    vmem = pl.BlockSpec(memory_space=pltpu.VMEM)
    anywhere = pl.BlockSpec(memory_space=pltpu.HBM)
    wire = cells // 2 + cells // 8
    dma = pltpu.SemaphoreType.DMA
    eigvecs, residuals, norms = pl.pallas_call(
        functools.partial(kernel, count, planes, cells, vector_part),
        out_shape=(
            pltpu.VMEM((vector_part, rows_local), jnp.bfloat16),
            pltpu.VMEM((vector_part, rows_local), jnp.bfloat16),
            pltpu.VMEM((1, vector_part), jnp.float32),
        ),
        in_specs=[anywhere] * 9,
        out_specs=(vmem, vmem, vmem),
        scratch_shapes=[
            pltpu.VMEM((rank_part, rows_local), jnp.bfloat16),
            pltpu.VMEM((rank_part, rows_local), jnp.bfloat16),
            pltpu.VMEM((planes, PAD, wire), jnp.bfloat16),
            pltpu.VMEM((planes, PAD, wire), jnp.bfloat16),
            pltpu.VMEM((planes + 2, PAD, cells + 2 * LANES), jnp.float32),
            pltpu.VMEM((2, PAD, cells), jnp.bfloat16),
            pltpu.VMEM((2, PAD, cells), jnp.bfloat16),
            pltpu.VMEM((8, slots), jnp.int32),
            pltpu.VMEM((2, PAD, cells), jnp.float32),
            pltpu.VMEM((cells // LANES * PAD, LANES), jnp.float32),
            pltpu.VMEM((2 * PAD, LANES), jnp.float32),
            pltpu.VMEM((count, 1, LANES), jnp.float32),
            pltpu.VMEM((8, slots), jnp.int32),
            pltpu.VMEM((2, 2 * PAD, rank_part), jnp.bfloat16),
            pltpu.VMEM((1, rows_local), jnp.float32),
            pltpu.VMEM((1, rows_local), jnp.float32),
            pltpu.VMEM((1, rows_local), jnp.float32),
            pltpu.VMEM((1, LANES), jnp.float32),
            pltpu.VMEM(coefficients.shape[::-1], jnp.bfloat16),
            pltpu.VMEM((1, vector_part), jnp.float32),
            pltpu.SMEM((1,), jnp.int32),
            pltpu.VMEM((1, slots), jnp.int32),
            pltpu.VMEM((1, slots), jnp.int32),
            dma((8,)),
            dma((planes,)),
            dma((planes,)),
            dma((planes,)),
            dma((planes,)),
            dma((planes,)),
            dma((3,)),
            dma((3,)),
            dma((count,)),
            dma((count,)),
        ],
        compiler_params=pltpu.CompilerParams(
            collective_id=0, has_side_effects=True, vmem_limit_bytes=56 * 1024 * 1024
        ),
    )(
        basis,
        coefficients.T,
        eigen_values[None, :],
        stiffness[None, :],
        damping[None, :],
        mass[None, :],
        link_count,
        lower_cells,
        upper_cells,
    )
    eigvecs, residuals, norms = pl.pallas_call(
        write_back,
        out_shape=tuple(
            jax.ShapeDtypeStruct(held.shape, held.dtype) for held in (eigvecs, residuals, norms)
        ),
        in_specs=[vmem] * 3,
        out_specs=[pl.BlockSpec(memory_space=pl.ANY)] * 3,
        scratch_shapes=[dma((3,))],
        compiler_params=pltpu.CompilerParams(vmem_limit_bytes=1 << 20),
    )(eigvecs, residuals, norms)
    return eigvecs, residuals, norms[0]


def solution(mesh):
    placed = (
        P("vecs", "rows"),
        P(),
        P("vecs"),
        P("rows"),
        P("rows"),
        P("rows"),
        P("rows"),
        P("rows", None),
        P("rows", None),
    )
    return jax.shard_map(
        on_device,
        mesh=mesh,
        in_specs=placed,
        out_specs=(P("vecs", "rows"), P("vecs", "rows"), P("vecs")),
        check_vma=False,
    )
```
